512 devices in a mesh: dp: 8 (over x, core), expert: 64 (over y, z).
Axes of the slice: x: 4, y: 8, z: 8, core: 2. Of those that a mesh axis runs over, the one named last changes fastest.
Arguments:
- grad_out: bfloat16 [65536, 2048], P(('dp', 'expert')), may hold values from -6 to 6
- expert_ids: int32 [65536, 6], P(('dp', 'expert')), may hold values from 0 to 63, all different within a row; in each aligned block of 128 rows (0 to 127, 128 to 255, ...) at most 16 rows name the same one
- gates: bfloat16 [65536, 6], P(('dp', 'expert')), may hold values from 0.049804688 to 1
- hidden: bfloat16 [524288, 704], P(('dp', 'expert')), may hold values from -6 to 6
- w_down: bfloat16 [64, 2048, 704], P('expert', 'dp'), may hold values from -0.21875 to 0.21875
Outputs:
- grad_hidden: bfloat16 [524288, 704], P(('dp', 'expert'))
- grad_down: float32 [64, 2048, 704], P('expert', 'dp')
- grad_gates: float32 [65536, 6], P(('dp', 'expert'))
The draws below stay inside these ranges and needn't reach their ends.
Inputs may be any that keep to these rules, and one draw needn't show every extreme that they name: `expert_ids`: in the rows of one device no expert is named by more than 16 rows; in every draw some device has an expert named by exactly 16 of its rows. A row names 6 different experts.
All inputs are finite; a program needn't handle non-finite values.
Results may differ from the reference program's by a relative error of at most 0.012.
Values may be sent and summed in bfloat16 or wider, within the bound.
No kernel may reach another device: no remote copies, remote signals or barrier semaphores. Data moves between devices by JAX's collectives and lax.ppermute only.
A program may use at most 64 MiB of HBM per device.

```python
import math
import jax
import jax.numpy as jnp
import numpy as np
from jax import lax

D = 2048
FF_W = 704
TOP = 6
TOK_DEV = 128
EXPERTS = 64
CAP = 16
TOKENS = 65536
SLOTS = 524288
N_DP = 8
N_EXPERT = 64


def block_scale(rng, shape, split, low, top_value):
    def one(position, parts):
        draws = jax.random.uniform(jax.random.fold_in(jax.random.fold_in(rng, 6), position), (parts,), jnp.float32, low / len(split), top_value / len(split))
        return jnp.repeat(jnp.exp(draws), shape[position] // parts).reshape((-1,) + (1,) * (len(shape) - position - 1))

    gain = one(*split[0])
    for cut in split[1:]:
        gain = gain * one(*cut)
    return gain


def deal_out(rng, own, number, rows, amount, top, limit, lean):
    sequence = jax.random.permutation(rng, amount)
    crowded, ordinary = portions_of(amount, rows * top, limit, lean, True), portions_of(amount, rows * top, limit, lean, False)
    places = jnp.arange(amount)

    def named(sizes, rotation):
        used = int((sizes > 0).sum())
        fixed = max(1, used // 4)
        moved = fixed + (places - fixed + rotation * (used - fixed)) % max(1, amount - fixed)
        return jnp.zeros((amount,), jnp.int32).at[sequence[jnp.where(places < fixed, places, moved)]].set(jnp.asarray(sizes, jnp.int32))

    sizes = jnp.where(number % 4 == 0, named(crowded, number // 4), named(ordinary, number - number // 4 - 1))
    mixed = jax.random.permutation(jax.random.fold_in(own, 3), amount)
    source_of, taker = mixed[0:amount // 2 * 2:2], mixed[1:amount // 2 * 2:2]
    slack = jnp.minimum(sizes[source_of] - 1, limit - sizes[taker]) // 2
    slack = jnp.where((source_of == sequence[0]) | (taker == sequence[0]) | (sizes[taker] == 0), 0, jnp.maximum(slack, 0))
    moved = jax.random.randint(jax.random.fold_in(own, 4), (amount // 2,), 0, 1 << 20) % (slack + 1)
    sizes = sizes.at[source_of].add(-moved).at[taker].add(moved)
    members = jnp.searchsorted(jnp.cumsum(sizes), jnp.arange(rows * top), side="right").astype(jnp.int32)
    grid = members.reshape(top, rows).T
    grid = grid[jax.random.permutation(jax.random.fold_in(own, 1), rows)]
    rotation = jax.random.randint(jax.random.fold_in(own, 2), (rows, 1), 0, top)
    return jnp.take_along_axis(grid, (jnp.arange(top)[None, :] + rotation) % top, axis=1)


def portions_of(number_of, total, bound, lean, full):
    loads = [(1 << 20) // math.isqrt(rank ** lean) + 1 for rank in range(1, number_of + 1)]
    largest = bound if full else min(bound, max(-(-total // number_of), total * loads[0] // sum(loads)))
    least = 1 if total - largest >= number_of - 1 else 0
    counts, surplus = [largest] + [least] * (number_of - 1), total - largest - least * (number_of - 1)
    while surplus > 0:
        movable = [i for i in range(1, number_of) if counts[i] < largest] or [i for i in range(1, number_of) if counts[i] < bound]
        pool, remaining = sum([loads[i] for i in movable]), surplus
        for i in movable:
            extra = min(bound - counts[i], max(1, remaining * loads[i] // pool), surplus)
            counts[i] = counts[i] + extra
            surplus = surplus - extra
    return np.array(counts)


def bell_draw(own_key, extent, scale, limit, pieces=(), kind=jnp.bfloat16):
    drawn = jax.random.normal(own_key, extent, jnp.float32) * scale
    if len(pieces) > 0:
        drawn = block_scale(own_key, extent, pieces, -0.22, 0.18) * drawn
    return jnp.clip(drawn, min=-limit, max=limit).astype(kind)


def setup_inputs(seed: int = 0) -> dict:
    key_list = jax.random.split(jax.random.key(seed), 6)
    grad_out = bell_draw(key_list[0], (TOKENS, D), 1.0, 6.0, ((0, 512),))
    expert_ids_keys = jax.random.split(jax.random.fold_in(key_list[1], 1), TOKENS // TOK_DEV)
    expert_ids_turns = jax.random.permutation(jax.random.fold_in(key_list[1], 3), TOKENS // TOK_DEV)
    expert_ids = jax.vmap(lambda own, number: deal_out(jax.random.fold_in(key_list[1], 2), own, number, TOK_DEV, EXPERTS, TOP, CAP, 2))(expert_ids_keys, expert_ids_turns).reshape((TOKENS, TOP))
    gates = jnp.clip(0.049804688 + 0.9501953 * jax.random.uniform(key_list[2], (TOKENS, TOP), jnp.float32) ** block_scale(key_list[2], (TOKENS, TOP), ((0, 512),), -0.2, 0.2), 0.049804688, 1.0).astype(jnp.bfloat16)
    hidden = bell_draw(key_list[3], (SLOTS, FF_W), 1.0, 6.0, ((0, 512),))
    w_down = bell_draw(key_list[4], (EXPERTS, D, FF_W), FF_W ** -0.5, 0.21875, ((0, 64), (1, 8)))
    return dict(grad_out=grad_out, expert_ids=expert_ids, gates=gates, hidden=hidden, w_down=w_down)


def block_ranks(ids_flat):
    onehot = (ids_flat[:, :, None] == jnp.arange(N_EXPERT, dtype=jnp.int32)[None, None, :]).astype(jnp.int32)
    before = jnp.cumsum(onehot, axis=1) - onehot
    return jnp.sum(before * onehot, axis=2).astype(jnp.int32)


def reference(grad_out, expert_ids, gates, hidden, w_down):
    blocks = N_DP * N_EXPERT
    ids_flat = expert_ids.reshape(blocks, TOK_DEV * TOP)
    ranks = block_ranks(ids_flat)
    block_of = jnp.arange(blocks, dtype=jnp.int32)
    dp_of = block_of // N_EXPERT
    src_of = block_of % N_EXPERT
    flat_pos = ((dp_of[:, None] * N_EXPERT + ids_flat) * N_EXPERT + src_of[:, None]) * CAP + ranks
    tok_of = jnp.broadcast_to((jnp.arange(TOK_DEV * TOP, dtype=jnp.int32) // TOP)[None, :], flat_pos.shape)
    total = N_DP * N_EXPERT * N_EXPERT * CAP
    table_tok = jnp.zeros((total,), jnp.int32).at[flat_pos.reshape(-1)].set(tok_of.reshape(-1))
    table_gate = jnp.zeros((total,), jnp.bfloat16).at[flat_pos.reshape(-1)].set(gates.reshape(-1))
    table_live = jnp.zeros((total,), jnp.bfloat16).at[flat_pos.reshape(-1)].set(jnp.ones((blocks * TOK_DEV * TOP,), jnp.bfloat16))
    table_tok = table_tok.reshape(N_DP, N_EXPERT, N_EXPERT, CAP)
    table_gate = table_gate.reshape(N_DP, N_EXPERT, N_EXPERT * CAP)
    table_live = table_live.reshape(N_DP, N_EXPERT, N_EXPERT * CAP)
    dy_blocks = grad_out.reshape(N_DP, N_EXPERT, TOK_DEV, D)
    hid = hidden.reshape(N_DP, N_EXPERT, N_EXPERT * CAP, FF_W)

    def one_expert(e):
        weight = w_down[e]
        total_grad = jnp.zeros((D, FF_W), jnp.float32)
        hid_out = []
        slot_out = []
        for i in range(N_DP):
            toks = table_tok[i, e]
            rows = jax.vmap(lambda s, tk: dy_blocks[i, s][tk])(jnp.arange(N_EXPERT, dtype=jnp.int32), toks)
            rows = rows.reshape(N_EXPERT * CAP, D) * table_live[i, e][:, None]
            gate_row = table_gate[i, e].astype(jnp.float32)
            h_rows = hid[i, e]
            u = jnp.dot(rows, weight, preferred_element_type=jnp.float32)
            hid_out.append((gate_row[:, None] * u).astype(jnp.bfloat16))
            scaled = (gate_row[:, None] * rows.astype(jnp.float32)).astype(jnp.bfloat16)
            part = jnp.dot(scaled.T, h_rows, preferred_element_type=jnp.float32).astype(jnp.bfloat16)
            total_grad = total_grad + part.astype(jnp.float32)
            slot_out.append(jnp.sum(h_rows.astype(jnp.float32) * u, axis=1))
        return jnp.stack(hid_out), total_grad, jnp.stack(slot_out)

    grad_hid, grad_down, slot_grad = lax.map(one_expert, jnp.arange(N_EXPERT, dtype=jnp.int32))
    grad_hid = jnp.transpose(grad_hid, (1, 0, 2, 3)).reshape(total, FF_W)
    slot_grad = jnp.transpose(slot_grad, (1, 0, 2)).reshape(total)
    grad_gates = slot_grad[flat_pos.reshape(-1)].reshape(N_DP * N_EXPERT * TOK_DEV, TOP)
    return grad_hid, grad_down, grad_gates
```

```python
import jax
import jax.numpy as jnp
from jax import lax
from jax.experimental import pallas as pl
from jax.experimental.pallas import tpu as pltpu
from jax.sharding import PartitionSpec as P


SIDE = 8
CAP = 16
LINE = SIDE * CAP
CHIPS = 4


def move_y(a, k):
    pairs = [(y * SIDE + z, (y + k) % SIDE * SIDE + z) for y in range(SIDE) for z in range(SIDE)]
    return lax.ppermute(a, "expert", pairs)


def move_z(a, k):
    pairs = [(y * SIDE + z, y * SIDE + (z + k) % SIDE) for y in range(SIDE) for z in range(SIDE)]
    return lax.ppermute(a, "expert", pairs)


def move_x(a, k):
    return lax.ppermute(a, "dp", [(x * 2 + c, (x + k) % CHIPS * 2 + c) for x in range(CHIPS) for c in range(2)])


def swap_core(a):
    return lax.ppermute(a, "dp", [(x * 2 + c, x * 2 + 1 - c) for x in range(CHIPS) for c in range(2)])


def ring_gather(a, move):
    ahead, back, found = a, a, [a]
    for step in range(1, SIDE // 2 + 1):
        ahead = move(ahead, 1)
        found.append(ahead)
        if step < SIDE // 2:
            back = move(back, -1)
            found.append(back)
    return found


OFFSETS = [0, -1, 1, -2, 2, -3, 3, -4]


def route_kernel(place_ref, want_ref, *refs):
    blocks, out_ref = refs[:SIDE], refs[SIDE]
    tokens = LINE
    want = want_ref[...]
    row = lax.broadcasted_iota(jnp.int32, (SIDE, tokens), 0)
    spread = (
        lax.broadcasted_iota(jnp.int32, (LINE, LINE), 0) % CAP == lax.broadcasted_iota(jnp.int32, (LINE, LINE), 1)
    ).astype(jnp.float32)
    group = (
        lax.broadcasted_iota(jnp.int32, (SIDE, LINE), 0) == lax.broadcasted_iota(jnp.int32, (SIDE, LINE), 1) // CAP
    ).astype(jnp.bfloat16)
    picked_gates = [jnp.zeros((SIDE, tokens), jnp.float32) for _ in range(SIDE)]
    for d in range(SIDE):
        meta = blocks[d][LINE : LINE + 8, :].astype(jnp.float32)
        target = meta[:, 0:128] * CAP + meta[:, 128:256]
        gates = meta[:, 256:384]
        select = jnp.zeros((LINE, tokens), jnp.float32)
        weigh = jnp.zeros((LINE, tokens), jnp.float32)
        for k in range(6):
            hit = target[k : k + 1, :] == want
            select = jnp.where(hit, 1.0, select)
            weigh = jnp.where(hit, gates[k : k + 1, :], weigh)
        rows = jnp.dot(
            select.astype(jnp.bfloat16), blocks[d][0:LINE, :], preferred_element_type=jnp.float32
        ).astype(jnp.bfloat16)
        start = pl.multiple_of(place_ref[d] * CAP, CAP)
        for k in range(SIDE):
            out_ref[k, pl.ds(start, CAP), :] = rows[k * CAP : (k + 1) * CAP, :]
        column = jnp.sum(weigh, axis=1, keepdims=True) * spread
        lines = jnp.dot(group, column.astype(jnp.bfloat16), preferred_element_type=jnp.float32)
        for k in range(SIDE):
            picked_gates[k] = jnp.where(row == place_ref[d], lines[k : k + 1, :], picked_gates[k])
    for k in range(SIDE):
        out_ref[k, LINE : LINE + 8, 0:128] = picked_gates[k].astype(jnp.bfloat16)


def route(place, want, blocks):
    width = blocks[0].shape[1]
    return pl.pallas_call(
        route_kernel,
        out_shape=jax.ShapeDtypeStruct((SIDE, LINE + 8, width), jnp.bfloat16),
        in_specs=[pl.BlockSpec(memory_space=pltpu.SMEM)] + [pl.BlockSpec(memory_space=pltpu.VMEM)] * (SIDE + 1),
        out_specs=pl.BlockSpec(memory_space=pltpu.VMEM),
        cost_estimate=pl.CostEstimate(flops=2 * SIDE * LINE * LINE * width, bytes_accessed=4 * LINE * SIDE * width, transcendentals=0),
        name="route",
    )(place, want, *blocks)


def shards(grad_out, expert_ids, gates, hidden, w_down):
    bf16, f32, i32 = jnp.bfloat16, jnp.float32, jnp.int32
    experts = lax.axis_size("expert")
    tok_rows, width = grad_out.shape
    top_count = expert_ids.shape[1]
    slot_rows, units = hidden.shape
    half = width // 2
    me = lax.axis_index("expert")
    my_y, my_z = me // SIDE, me % SIDE
    dp = lax.axis_index("dp")
    my_x, my_c = dp // 2, dp % 2

    ids = expert_ids.T
    hot = ids[:, None, :] == jnp.arange(experts, dtype=i32)[None, :, None]
    named = jnp.sum(hot.astype(f32), axis=0).astype(bf16)
    token = jnp.arange(tok_rows, dtype=i32)
    earlier = (token[:, None] < token[None, :]).astype(bf16)
    before = jnp.dot(named, earlier, preferred_element_type=f32)
    ranks = jnp.sum(jnp.where(hot, before[None], 0.0), axis=1)
    pad = ((0, 8 - top_count), (0, 0))
    meta = jnp.concatenate(
        [
            jnp.pad(ids.astype(f32), pad, constant_values=-1.0),
            jnp.pad(ranks, pad),
            jnp.pad(gates.T.astype(f32), pad),
            jnp.zeros((8, half - 3 * tok_rows), f32),
        ],
        axis=1,
    ).astype(bf16)
    first = jnp.concatenate([grad_out[:, :half], meta], axis=0)
    second = jnp.concatenate([grad_out[:, half:], meta], axis=0)

    own_w = w_down[0]
    by_chip = jnp.zeros((CHIPS,) + own_w.shape, bf16)
    by_chip = lax.dynamic_update_slice(by_chip, own_w[None], (my_x, 0, 0))
    for k in range(1, CHIPS):
        by_chip = lax.dynamic_update_slice(by_chip, move_x(own_w, k)[None], ((my_x - k) % CHIPS, 0, 0))
    other = swap_core(by_chip)
    weight = jnp.zeros((CHIPS, 2) + own_w.shape, bf16)
    weight = lax.dynamic_update_slice(weight, by_chip[:, None], (0, my_c, 0, 0))
    weight = lax.dynamic_update_slice(weight, other[:, None], (0, 1 - my_c, 0, 0))
    weight = weight.reshape(width, units)

    along_y = ring_gather(first, move_y)
    along_z = ring_gather(second, move_z)
    offsets = jnp.array(OFFSETS, i32)
    slot = jnp.arange(LINE, dtype=i32)
    want_first = (my_y * SIDE + (my_z + slot // CAP) % SIDE) * CAP + slot % CAP
    want_second = ((my_y + slot // CAP) % SIDE * SIDE + my_z) * CAP + slot % CAP
    spread = lambda w: jnp.broadcast_to(w.astype(f32)[:, None], (LINE, tok_rows))
    out_first = route((my_y + offsets) % SIDE, spread(want_first), along_y)
    out_second = route((my_z + offsets) % SIDE, spread(want_second), along_z)
    rows = jnp.zeros((SIDE, SIDE, CAP, width), bf16)
    gate_all = jnp.zeros((SIDE, SIDE, CAP), bf16)
    for k in [0, 4, 3, 5, 2, 6, 1, 7]:
        got = out_first[k] if k == 0 else move_z(out_first[k], k)
        z = (my_z - k) % SIDE
        rows = lax.dynamic_update_slice(rows, got[:LINE].reshape(SIDE, 1, CAP, half), (0, z, 0, 0))
        gate_all = lax.dynamic_update_slice(gate_all, got[LINE:, :CAP][:, None], (0, z, 0))
        got = out_second[k, :LINE] if k == 0 else move_y(out_second[k, :LINE], k)
        rows = lax.dynamic_update_slice(rows, got.reshape(1, SIDE, CAP, half), ((my_y - k) % SIDE, 0, 0, half))

    dispatched = rows.reshape(slot_rows, width)
    gate_row = gate_all.reshape(slot_rows).astype(f32)
    scaled = (gate_row[:, None] * dispatched.astype(f32)).astype(bf16)
    partial = lax.dot_general(
        scaled, hidden, (((0,), (0,)), ((), ())), preferred_element_type=f32
    ).astype(bf16)
    u_rows = jnp.dot(dispatched, weight, preferred_element_type=f32)
    grad_hidden = (gate_row[:, None] * u_rows).astype(bf16)
    slot_grad = jnp.sum(hidden.astype(f32) * u_rows, axis=1)

    shares = partial.reshape((CHIPS, 2) + own_w.shape)
    keep = lax.dynamic_index_in_dim(shares, my_c, axis=1, keepdims=False)
    give = lax.dynamic_index_in_dim(shares, 1 - my_c, axis=1, keepdims=False)
    both = keep.astype(f32) + swap_core(give).astype(f32)
    grad_down = lax.dynamic_index_in_dim(both, my_x, axis=0, keepdims=False)
    for k in [2, 1, 3]:
        sent = lax.dynamic_index_in_dim(both, (my_x + k) % CHIPS, axis=0, keepdims=False).astype(bf16)
        grad_down = grad_down + move_x(sent, k).astype(f32)

    returned = lax.all_to_all(
        slot_grad.reshape(experts, CAP), "expert", split_axis=0, concat_axis=0, tiled=True
    )
    target = ids * CAP + ranks.astype(i32)
    grad_gates = jnp.take(returned.reshape(-1), target.T.reshape(-1)).reshape(tok_rows, top_count)
    return (grad_hidden, grad_down[None], grad_gates)


def solution(mesh):
    return jax.shard_map(
        shards,
        mesh=mesh,
        in_specs=(
            P(("dp", "expert"), None),
            P(("dp", "expert"), None),
            P(("dp", "expert"), None),
            P(("dp", "expert"), None),
            P("expert", "dp", None),
        ),
        out_specs=(P(("dp", "expert"), None), P("expert", "dp", None), P(("dp", "expert"), None)),
        check_vma=False,
    )
```

```python
import jax
import jax.numpy as jnp
from jax import lax
from jax.experimental import pallas as pl
from jax.experimental.pallas import tpu as pltpu
from jax.sharding import PartitionSpec as P


SIDE = 8
CAP = 16
LINE = SIDE * CAP
CHIPS = 4
LANES = 128
TOP = 6
OFFSETS = [0, -1, 1, -2, 2, -3, 3, -4]
EARLY, LATE = [0, 4, 1, 7, 3, 2], [6, 5]
VMEM = pl.BlockSpec(memory_space=pltpu.VMEM)
SMEM = pl.BlockSpec(memory_space=pltpu.SMEM)


def move_x(a, k):
    return lax.ppermute(a, "dp", [(x * 2 + c, (x + k) % CHIPS * 2 + c) for x in range(CHIPS) for c in range(2)])


def swap_core(a):
    return lax.ppermute(a, "dp", [(x * 2 + c, x * 2 + 1 - c) for x in range(CHIPS) for c in range(2)])


def move_plane(a, k, first_axis):
    pairs = []
    for dp in range(2 * CHIPS):
        for y in range(SIDE):
            for z in range(SIDE):
                to = ((y + k) % SIDE, z) if dp % 2 == first_axis else (y, (z + k) % SIDE)
                pairs.append(((dp * SIDE + y) * SIDE + z, (dp * SIDE + to[0]) * SIDE + to[1]))
    return lax.ppermute(a, ("dp", "expert"), pairs)


def exchange(a):
    return lax.all_to_all(a, "expert", split_axis=0, concat_axis=0, tiled=True)


def head_kernel(place_ref, ids_ref, gates_ref, tokens_ref, own_ref, other_ref, target_ref):
    tokens, share = tokens_ref.shape[0], tokens_ref.shape[1] // (2 * CHIPS)
    experts = SIDE * SIDE
    row = lax.broadcasted_iota(jnp.int32, (tokens, tokens), 0)
    earlier = (row < lax.broadcasted_iota(jnp.int32, (tokens, tokens), 1)).astype(jnp.bfloat16)
    expert = lax.broadcasted_iota(jnp.int32, (experts, tokens), 0)
    hot = [(expert == ids_ref[k : k + 1, :]).astype(jnp.float32) for k in range(TOP)]
    before = jnp.dot(sum(hot).astype(jnp.bfloat16), earlier, preferred_element_type=jnp.float32)
    ranks = [jnp.sum(h * before, axis=0, keepdims=True) for h in hot]
    blank = jnp.zeros((2, tokens), jnp.float32)
    ids = jnp.concatenate([ids_ref[...].astype(jnp.float32), blank - 1.0], axis=0)
    ranks = jnp.concatenate(ranks + [blank], axis=0)
    gates = jnp.concatenate([gates_ref[...].astype(jnp.float32), blank], axis=0)
    target_ref[...] = (ids * CAP + ranks).astype(jnp.int32)
    for half, out_ref in enumerate((own_ref, other_ref)):
        for b in range(CHIPS):
            start = pl.multiple_of(place_ref[half * CHIPS + b] * share, share)
            out_ref[0:tokens, b * share : (b + 1) * share] = tokens_ref[:, pl.ds(start, share)]
        for n, part in enumerate((ids, ranks, gates)):
            out_ref[tokens : tokens + 8, n * tokens : (n + 1) * tokens] = part.astype(jnp.bfloat16)
        out_ref[tokens : tokens + 8, 3 * tokens :] = jnp.zeros(
            (8, out_ref.shape[1] - 3 * tokens), jnp.bfloat16
        )


def route_kernel(place_ref, want_ref, *refs):
    blocks, outs = refs[:SIDE], refs[SIDE:]
    want = want_ref[...]
    ones = jnp.ones((LINE, LANES), jnp.bfloat16)
    for d in range(SIDE):
        place = place_ref[d]
        for i in range(2):
            meta = blocks[d][i, LINE : LINE + 8, 0 : 3 * LINE].astype(jnp.float32)
            target = meta[:, 0:LINE] * CAP + meta[:, LINE : 2 * LINE]
            gates = meta[:, 2 * LINE : 3 * LINE]
            select = jnp.zeros((LINE, LINE), jnp.float32)
            weigh = jnp.zeros((LINE, LINE), jnp.float32)
            for k in range(TOP):
                hit = target[k : k + 1, :] == want
                select = jnp.where(hit, 1.0, select)
                if i == 0:
                    weigh = jnp.where(hit, gates[k : k + 1, :], weigh)
            rows = jnp.dot(
                select.astype(jnp.bfloat16), blocks[d][i, 0:LINE, :], preferred_element_type=jnp.float32
            ).astype(jnp.bfloat16)
            start = pl.multiple_of(i * LINE + place * CAP, CAP)
            for k in range(SIDE):
                outs[k][pl.ds(start, CAP), :] = rows[k * CAP : (k + 1) * CAP, :]
            if i == 0:
                wide = jnp.dot(weigh.astype(jnp.bfloat16), ones, preferred_element_type=jnp.float32)
                wide = wide.astype(jnp.bfloat16)
                lane = pl.multiple_of(place * LANES, LANES)
                for k in range(SIDE):
                    outs[k][2 * LINE :, pl.ds(lane, LANES)] = wide[k * CAP : (k + 1) * CAP, :]


def join_kernel(slots_ref, *refs):
    kept, early_ref, late_ref = refs[:SIDE], refs[SIDE], refs[SIDE + 1]
    rows_ref, scaled_ref, gate_ref = refs[SIDE + 2 :]
    half = rows_ref.shape[1] // 2
    for k in range(SIDE):
        for j in range(SIDE):
            slot = pl.ds(pl.multiple_of(slots_ref[0, k * SIDE + j] * CAP, CAP), CAP)
            gate = kept[k][2 * LINE :, j * LANES : (j + 1) * LANES]
            rows = kept[k][j * CAP : (j + 1) * CAP, :]
            gate_ref[slot, :] = gate
            rows_ref[slot, 0:half] = rows
            scaled_ref[slot, 0:half] = rows * jnp.concatenate([gate] * (half // LANES), axis=1)
    for ref, order in ((early_ref, EARLY), (late_ref, LATE)):
        for n, k in enumerate(order):
            for j in range(SIDE):
                slot = pl.ds(pl.multiple_of(slots_ref[1, k * SIDE + j] * CAP, CAP), CAP)
                rows = ref[n, j * CAP : (j + 1) * CAP, :]
                rows_ref[slot, half:] = rows
                scaled_ref[slot, half:] = rows * jnp.concatenate([gate_ref[slot, :]] * (half // LANES), axis=1)


def pick_kernel(target_ref, table_ref, out_ref):
    experts, caps = table_ref.shape
    rest, pieces = table_ref[...], []
    for _ in range(3):
        piece = rest.astype(jnp.bfloat16)
        pieces.append(piece)
        rest = rest - piece.astype(jnp.float32)
    tokens = out_ref.shape[1]
    expert = lax.broadcasted_iota(jnp.int32, (experts, tokens), 0)
    cap = lax.broadcasted_iota(jnp.int32, (caps, tokens), 0)
    for k in range(out_ref.shape[0]):
        target = target_ref[k : k + 1, :]
        hot = (expert == target // caps).astype(jnp.bfloat16)
        found = sum(
            lax.dot_general(p, hot, (((0,), (0,)), ((), ())), preferred_element_type=jnp.float32) for p in pieces
        )
        out_ref[k : k + 1, :] = jnp.sum(jnp.where(cap == target % caps, found, 0.0), axis=0, keepdims=True)


def pick(target, table):
    return pl.pallas_call(
        pick_kernel,
        out_shape=jax.ShapeDtypeStruct(target.shape, jnp.float32),
        in_specs=[pl.BlockSpec(memory_space=pltpu.VMEM)] * 2,
        out_specs=pl.BlockSpec(memory_space=pltpu.VMEM),
        name="pick",
    )(target, table)


def shards(grad_out, expert_ids, gates, hidden, w_down):
    bf16, f32, i32 = jnp.bfloat16, jnp.float32, jnp.int32
    experts = lax.axis_size("expert")
    tok_rows, width = grad_out.shape
    slot_rows, units = hidden.shape
    half = width // 2
    me, dp = lax.axis_index("expert"), lax.axis_index("dp")
    my_y, my_z, my_x, my_c = me // SIDE, me % SIDE, dp // 2, dp % 2
    along = jnp.where(my_c == 0, my_y, my_z)
    across = jnp.where(my_c == 0, my_z, my_y)

    b = jnp.arange(2 * CHIPS, dtype=i32)
    place = (my_x + b % CHIPS) % CHIPS * 2 + (my_c + b // CHIPS) % 2
    block = jax.ShapeDtypeStruct((tok_rows + 8, half), bf16)
    own, other, target = pl.pallas_call(
        head_kernel,
        out_shape=(block, block, jax.ShapeDtypeStruct((8, tok_rows), i32)),
        in_specs=[SMEM, VMEM, VMEM, VMEM],
        out_specs=(VMEM,) * 3,
        name="head",
    )(place, expert_ids.T, gates.T, grad_out)

    lent = swap_core(other)
    pair = jnp.stack([own, lent])
    minus_2, plus_2 = move_plane(pair, 2, 0), move_plane(pair, -2, 0)
    minus_1, plus_1 = move_plane(pair, 1, 0), move_plane(pair, -1, 0)
    minus_4 = move_plane(minus_2, 2, 0)
    minus_3, plus_3 = move_plane(minus_2, 1, 0), move_plane(plus_2, -1, 0)
    found = [pair, minus_1, plus_1, minus_2, plus_2, minus_3, plus_3, minus_4]

    slot = jnp.arange(LINE, dtype=i32)
    step, cap = (across + slot // CAP) % SIDE, slot % CAP
    want = jnp.where(my_c == 0, my_y * SIDE + step, step * SIDE + my_z) * CAP + cap
    routed = pl.pallas_call(
        route_kernel,
        out_shape=(jax.ShapeDtypeStruct((2 * LINE + CAP, half), bf16),) * SIDE,
        in_specs=[SMEM] + [VMEM] * (SIDE + 1),
        out_specs=(VMEM,) * SIDE,
        name="route",
    )((along + jnp.array(OFFSETS, i32)) % SIDE, jnp.broadcast_to(want.astype(f32)[:, None], (LINE, tok_rows)), *found)
    kept = list(routed)
    for k in [4, 3, 5, 2, 6, 1, 7]:
        kept[k] = move_plane(routed[k], k, 1)
    early = swap_core(jnp.stack([kept[k][LINE : 2 * LINE] for k in EARLY]))
    late = swap_core(jnp.stack([kept[k][LINE : 2 * LINE] for k in LATE]))
    k, j = jnp.arange(SIDE, dtype=i32)[:, None], jnp.arange(SIDE, dtype=i32)[None, :]
    by_z, by_y = j * SIDE + (my_z - k) % SIDE, (my_y - k) % SIDE * SIDE + j
    slots = jnp.stack([jnp.where(my_c == 0, by_z, by_y).reshape(-1), jnp.where(my_c == 0, by_y, by_z).reshape(-1)])
    full = jax.ShapeDtypeStruct((slot_rows, width), bf16)
    rows, scaled, gate_wide = pl.pallas_call(
        join_kernel,
        out_shape=(full, full, jax.ShapeDtypeStruct((slot_rows, LANES), bf16)),
        in_specs=[SMEM] + [VMEM] * (SIDE + 2),
        out_specs=(VMEM,) * 3,
        name="join",
    )(slots, *kept, early, late)
    gate_row = gate_wide[:, :1].astype(f32)

    own_w = w_down[0]
    moved = [move_x(own_w, -k) for k in range(1, CHIPS)]
    same_core = jnp.stack([own_w] + moved)
    other_core = swap_core(same_core)
    weight = jnp.concatenate([same_core, other_core]).reshape(width, units)

    def share_of(columns):
        product = lax.dot_general(columns, hidden, (((0,), (0,)), ((), ())), preferred_element_type=f32)
        return product.astype(bf16).reshape((CHIPS,) + own_w.shape)

    give = share_of(scaled[:, width // 2 :])
    other = swap_core(give)
    both = share_of(scaled[:, : width // 2]).astype(f32) + other.astype(f32)
    grad_down = both[0]
    for k in (2, 1, 3):
        moved = move_x(both[k].astype(bf16), k)
        grad_down = grad_down + moved.astype(f32)

    u_rows = jnp.dot(rows, weight, preferred_element_type=f32)
    grad_hidden = (gate_row * u_rows).astype(bf16)
    slot_grad = jnp.sum(hidden.astype(f32) * u_rows, axis=1)

    returned = exchange(slot_grad.reshape(experts, CAP))
    grad_gates = pick(target, returned)[:TOP].T
    return (grad_hidden, grad_down[None], grad_gates)


def solution(mesh):
    return jax.shard_map(
        shards,
        mesh=mesh,
        in_specs=(
            P(("dp", "expert"), None),
            P(("dp", "expert"), None),
            P(("dp", "expert"), None),
            P(("dp", "expert"), None),
            P("expert", "dp", None),
        ),
        out_specs=(P(("dp", "expert"), None), P("expert", "dp", None), P(("dp", "expert"), None)),
        check_vma=False,
    )
```

```python
import jax
import jax.numpy as jnp
from jax import lax
from jax.experimental import pallas as pl
from jax.experimental.pallas import tpu as pltpu
from jax.sharding import PartitionSpec as P


SIDE = 8
CAP = 16
LINE = SIDE * CAP
CHIPS = 4
LANES = 128
TOP = 6
OFFSETS = [0, -1, 1, -2, 2, -3, 3, -4]
EARLY, LATE = [0, 4, 1, 7, 3, 5], [6, 2]
VMEM = pl.BlockSpec(memory_space=pltpu.VMEM)
SMEM = pl.BlockSpec(memory_space=pltpu.SMEM)


def move_x(a, k):
    return lax.ppermute(a, "dp", [(x * 2 + c, (x + k) % CHIPS * 2 + c) for x in range(CHIPS) for c in range(2)])


def swap_core(a):
    return lax.ppermute(a, "dp", [(x * 2 + c, x * 2 + 1 - c) for x in range(CHIPS) for c in range(2)])


def move_plane(a, k, first_axis):
    pairs = []
    for dp in range(2 * CHIPS):
        for y in range(SIDE):
            for z in range(SIDE):
                to = ((y + k) % SIDE, z) if dp % 2 == first_axis else (y, (z + k) % SIDE)
                pairs.append(((dp * SIDE + y) * SIDE + z, (dp * SIDE + to[0]) * SIDE + to[1]))
    return lax.ppermute(a, ("dp", "expert"), pairs)


def exchange(a):
    return lax.all_to_all(a, "expert", split_axis=0, concat_axis=0, tiled=True)


def head_kernel(ids_ref, gates_ref, tokens_ref, pair_ref, other_ref, target_ref):
    tokens, share = tokens_ref.shape[0], tokens_ref.shape[1] // (2 * CHIPS)
    experts = SIDE * SIDE
    row = lax.broadcasted_iota(jnp.int32, (tokens, tokens), 0)
    earlier = (row < lax.broadcasted_iota(jnp.int32, (tokens, tokens), 1)).astype(jnp.bfloat16)
    expert = lax.broadcasted_iota(jnp.int32, (experts, tokens), 0)
    hot = [(expert == ids_ref[k : k + 1, :]).astype(jnp.float32) for k in range(TOP)]
    before = jnp.dot(sum(hot).astype(jnp.bfloat16), earlier, preferred_element_type=jnp.float32)
    ranks = [jnp.sum(h * before, axis=0, keepdims=True) for h in hot]
    blank = jnp.zeros((2, tokens), jnp.float32)
    ids = jnp.concatenate([ids_ref[...].astype(jnp.float32), blank - 1.0], axis=0)
    ranks = jnp.concatenate(ranks + [blank], axis=0)
    gates = jnp.concatenate([gates_ref[...].astype(jnp.float32), blank], axis=0)
    target_ref[...] = (ids * CAP + ranks)[0:TOP].astype(jnp.int32)
    dp = lax.axis_index("dp")
    for half, out_ref in enumerate((pair_ref.at[0], other_ref)):
        for b in range(CHIPS):
            place = lax.rem(dp // 2 + b, CHIPS) * 2 + lax.rem(dp + half, 2)
            start = pl.multiple_of(place * share, share)
            out_ref[0:tokens, b * share : (b + 1) * share] = tokens_ref[:, pl.ds(start, share)]
        for n, part in enumerate((ids, ranks, gates)):
            out_ref[tokens : tokens + 8, n * tokens : (n + 1) * tokens] = part.astype(jnp.bfloat16)
        out_ref[tokens : tokens + 8, 3 * tokens :] = jnp.zeros(
            (8, out_ref.shape[1] - 3 * tokens), jnp.bfloat16
        )


def route_kernel(place_ref, *refs):
    blocks, outs = refs[:SIDE], refs[SIDE:]
    line = lax.broadcasted_iota(jnp.int32, (LINE, LINE), 0)
    step = (place_ref[SIDE] + line // CAP) % SIDE
    want = ((step * place_ref[SIDE + 1] + place_ref[SIDE + 2]) * CAP + line % CAP).astype(jnp.float32)
    ones = jnp.ones((LINE, LANES), jnp.bfloat16)
    for d in range(SIDE):
        place = place_ref[d]
        for i in range(2):
            meta = blocks[d][i, LINE : LINE + 8, 0 : 3 * LINE].astype(jnp.float32)
            target = meta[:, 0:LINE] * CAP + meta[:, LINE : 2 * LINE]
            gates = meta[:, 2 * LINE : 3 * LINE]
            select = jnp.zeros((LINE, LINE), jnp.float32)
            weigh = jnp.zeros((LINE, LINE), jnp.float32)
            for k in range(TOP):
                hit = target[k : k + 1, :] == want
                select = jnp.where(hit, 1.0, select)
                if i == 0:
                    weigh = jnp.where(hit, gates[k : k + 1, :], weigh)
            rows = jnp.dot(
                select.astype(jnp.bfloat16), blocks[d][i, 0:LINE, :], preferred_element_type=jnp.float32
            ).astype(jnp.bfloat16)
            start = pl.multiple_of(i * LINE + place * CAP, CAP)
            for k in range(SIDE):
                outs[k][pl.ds(start, CAP), :] = rows[k * CAP : (k + 1) * CAP, :]
            if i == 0:
                wide = jnp.dot(weigh.astype(jnp.bfloat16), ones, preferred_element_type=jnp.float32)
                wide = wide.astype(jnp.bfloat16)
                lane = pl.multiple_of(place * LANES, LANES)
                for k in range(SIDE):
                    outs[k][2 * LINE :, pl.ds(lane, LANES)] = wide[k * CAP : (k + 1) * CAP, :]


def join_kernel(slots_ref, *refs):
    kept, early_ref, late_ref = refs[:SIDE], refs[SIDE], refs[SIDE + 1]
    rows_ref, scaled_ref, gate_ref = refs[SIDE + 2 :]
    half = rows_ref.shape[1] // 2
    for k in range(SIDE):
        for j in range(SIDE):
            slot = pl.ds(pl.multiple_of(slots_ref[0, k * SIDE + j] * CAP, CAP), CAP)
            gate = kept[k][2 * LINE :, j * LANES : (j + 1) * LANES]
            rows = kept[k][j * CAP : (j + 1) * CAP, :]
            gate_ref[slot, :] = gate
            rows_ref[slot, 0:half] = rows
            scaled_ref[slot, 0:half] = rows * jnp.concatenate([gate] * (half // LANES), axis=1)
    for ref, order in ((early_ref, EARLY), (late_ref, LATE)):
        for n, k in enumerate(order):
            for j in range(SIDE):
                slot = pl.ds(pl.multiple_of(slots_ref[1, k * SIDE + j] * CAP, CAP), CAP)
                rows = ref[n, j * CAP : (j + 1) * CAP, :]
                rows_ref[slot, half:] = rows
                scaled_ref[slot, half:] = rows * jnp.concatenate([gate_ref[slot, :]] * (half // LANES), axis=1)


def pick_kernel(target_ref, table_ref, out_ref):
    experts, caps = table_ref.shape
    rest, pieces = table_ref[...], []
    for _ in range(3):
        piece = rest.astype(jnp.bfloat16)
        pieces.append(piece)
        rest = rest - piece.astype(jnp.float32)
    tokens = out_ref.shape[1]
    expert = lax.broadcasted_iota(jnp.int32, (experts, tokens), 0)
    cap = lax.broadcasted_iota(jnp.int32, (caps, tokens), 0)
    for k in range(out_ref.shape[0]):
        target = target_ref[k : k + 1, :]
        hot = (expert == target // caps).astype(jnp.bfloat16)
        found = sum(
            lax.dot_general(p, hot, (((0,), (0,)), ((), ())), preferred_element_type=jnp.float32) for p in pieces
        )
        out_ref[k : k + 1, :] = jnp.sum(jnp.where(cap == target % caps, found, 0.0), axis=0, keepdims=True)


def pick(target, table):
    return pl.pallas_call(
        pick_kernel,
        out_shape=jax.ShapeDtypeStruct(target.shape, jnp.float32),
        in_specs=[pl.BlockSpec(memory_space=pltpu.VMEM)] * 2,
        out_specs=pl.BlockSpec(memory_space=pltpu.VMEM),
        name="pick",
    )(target, table)


def shards(grad_out, expert_ids, gates, hidden, w_down):
    bf16, f32, i32 = jnp.bfloat16, jnp.float32, jnp.int32
    experts = lax.axis_size("expert")
    tok_rows, width = grad_out.shape
    slot_rows, units = hidden.shape
    half = width // 2
    me, dp = lax.axis_index("expert"), lax.axis_index("dp")
    my_y, my_z, my_c = me // SIDE, me % SIDE, dp % 2
    along = jnp.where(my_c == 0, my_y, my_z)
    across = jnp.where(my_c == 0, my_z, my_y)

    block = (tok_rows + 8, half)
    pair, other, target = pl.pallas_call(
        head_kernel,
        out_shape=(
            jax.ShapeDtypeStruct((2,) + block, bf16),
            jax.ShapeDtypeStruct(block, bf16),
            jax.ShapeDtypeStruct((TOP, tok_rows), i32),
        ),
        in_specs=[VMEM, VMEM, VMEM],
        out_specs=(VMEM,) * 3,
        name="head",
    )(expert_ids.T, gates.T, grad_out)

    lent = swap_core(other)
    pair = lax.dynamic_update_slice(pair, lent[None], (1, 0, 0))
    minus_2, plus_2 = move_plane(pair, 2, 0), move_plane(pair, -2, 0)
    minus_1, plus_1 = move_plane(pair, 1, 0), move_plane(pair, -1, 0)
    minus_4 = move_plane(minus_2, 2, 0)
    minus_3, plus_3 = move_plane(minus_2, 1, 0), move_plane(plus_2, -1, 0)
    found = [pair, minus_1, plus_1, minus_2, plus_2, minus_3, plus_3, minus_4]

    stride = jnp.where(my_c == 0, 1, SIDE)
    origin = jnp.where(my_c == 0, my_y * SIDE, my_z)
    spots = (along + jnp.array(OFFSETS + [0] * 3, i32)) % SIDE
    n = jnp.arange(SIDE + 3, dtype=i32)
    spots = jnp.where(n == SIDE, across, jnp.where(n == SIDE + 1, stride, jnp.where(n == SIDE + 2, origin, spots)))
    routed = pl.pallas_call(
        route_kernel,
        out_shape=(jax.ShapeDtypeStruct((2 * LINE + CAP, half), bf16),) * SIDE,
        in_specs=[SMEM] + [VMEM] * SIDE,
        out_specs=(VMEM,) * SIDE,
        name="route",
    )(spots, *found)
    kept = list(routed)
    for k in [3, 5, 4, 2, 6, 1, 7]:
        kept[k] = move_plane(routed[k], k, 1)
    early = swap_core(jnp.stack([kept[k][LINE : 2 * LINE] for k in EARLY]))
    late = swap_core(jnp.stack([kept[k][LINE : 2 * LINE] for k in LATE]))
    k, j = jnp.arange(SIDE, dtype=i32)[:, None], jnp.arange(SIDE, dtype=i32)[None, :]
    by_z, by_y = j * SIDE + (my_z - k) % SIDE, (my_y - k) % SIDE * SIDE + j
    slots = jnp.stack([jnp.where(my_c == 0, by_z, by_y).reshape(-1), jnp.where(my_c == 0, by_y, by_z).reshape(-1)])
    full = jax.ShapeDtypeStruct((slot_rows, width), bf16)
    rows, scaled, gate_wide = pl.pallas_call(
        join_kernel,
        out_shape=(full, full, jax.ShapeDtypeStruct((slot_rows, LANES), bf16)),
        in_specs=[SMEM] + [VMEM] * (SIDE + 2),
        out_specs=(VMEM,) * 3,
        name="join",
    )(slots, *kept, early, late)
    gate_row = gate_wide[:, :1].astype(f32)

    own_w = w_down[0]
    moved = [move_x(own_w, -k) for k in range(1, CHIPS)]
    same_core = jnp.stack([own_w] + moved)
    other_core = swap_core(same_core)
    weight = jnp.concatenate([same_core, other_core]).reshape(width, units)

    def share_of(columns):
        product = lax.dot_general(columns, hidden, (((0,), (0,)), ((), ())), preferred_element_type=f32)
        return product.astype(bf16).reshape((CHIPS,) + own_w.shape)

    give = share_of(scaled[:, width // 2 :])
    other = swap_core(give)
    both = share_of(scaled[:, : width // 2]).astype(f32) + other.astype(f32)
    grad_down = both[0]
    for k in (2, 1, 3):
        moved = move_x(both[k].astype(bf16), k)
        grad_down = grad_down + moved.astype(f32)

    u_rows = jnp.dot(rows, weight, preferred_element_type=f32)
    grad_hidden = (gate_row * u_rows).astype(bf16)
    slot_grad = jnp.sum(hidden.astype(f32) * u_rows, axis=1)

    returned = exchange(slot_grad.reshape(experts, CAP))
    grad_gates = pick(target, returned).T
    return (grad_hidden, grad_down[None], grad_gates)


def solution(mesh):
    return jax.shard_map(
        shards,
        mesh=mesh,
        in_specs=(
            P(("dp", "expert"), None),
            P(("dp", "expert"), None),
            P(("dp", "expert"), None),
            P(("dp", "expert"), None),
            P("expert", "dp", None),
        ),
        out_specs=(P(("dp", "expert"), None), P("expert", "dp", None), P(("dp", "expert"), None)),
        check_vma=False,
    )
```
